32 devices in a mesh: elem: 8 (over z, x), blk: 4 (over y, core).
Axes of the slice: x: 2, y: 2, z: 4, core: 2. Of those that a mesh axis runs over, the one named last changes fastest.
Arguments:
- diagonal_block_list: bfloat16 [32, 512, 512], P('elem', None, 'blk'), may hold values from -0.25 to 0.25
- neighbour_block_list: bfloat16 [32, 6, 512, 512], P('elem', None, None, 'blk'), may hold values from -0.25 to 0.25
- neighbours: int32 [32, 6], P('elem'), may hold values from 0 to 31, as said below
- damping: float32 [32, 512], P('elem', 'blk'), may hold values from 0.05 to 0.3
- bases: bfloat16 [32, 512, 128], P('elem', 'blk'), may hold values from -1.1953125 to 1.1953125
- agglomerate: int32 [32], replicated, may hold values from 0 to 15, as said below
- group: int32 [16], replicated, may hold values from 0 to 7
Outputs:
- smoothed: bfloat16 [32, 512, 128], P('elem', 'blk')
- coarse: float32 [16, 128, 128], P('elem', 'blk')
- last_level: float32 [8, 128, 128], P(None, 'blk')
The draws below stay inside these ranges and needn't reach their ends.
Inputs may be any that keep to these rules, and one draw needn't show every extreme that they name: `neighbours`: each neighbour lies on the same index of elem as its element or on the next index on either side; every index of elem has a neighbour on an adjacent index. The elements of one agglomerate are consecutive; every agglomerate has one element or more.
All inputs are finite; a program needn't handle non-finite values.
Results may differ from the reference program's by a relative error of at most 0.007.
Values may be sent and summed in bfloat16 or wider, within the bound.
No kernel may reach another device: no remote copies, remote signals or barrier semaphores. Data moves between devices by JAX's collectives and lax.ppermute only.
A program may use at most 64 MiB of HBM per device.

```python
import math
import jax
import jax.numpy as jnp
from jax import lax

NB = 512
NC = 128
NBR = 6
SWEEPS = 2
NG = 8
E_DEV = 4
NE = 32
NAGG = 16
N_ELEM = 8


def draw_neighbours(key, part):
    key_side = jax.random.fold_in(key, 11)
    key_local = jax.random.fold_in(key, 12)
    element = jnp.arange(NE, dtype=jnp.int32)
    device = element // E_DEV
    offset = jax.random.randint(key_side, (NE, NBR), -1, 2)
    target = jnp.clip(device[:, None] + offset, 0, N_ELEM - 1)
    forced = jnp.where(device + 1 < N_ELEM, device + 1, device - 1)
    is_first = (element % E_DEV == 0)[:, None] & (jnp.arange(NBR)[None, :] == 0)
    target = jnp.where(is_first, forced[:, None], target)
    local_index = jax.random.randint(key_local, (NE, NBR), 0, E_DEV)
    return (target * E_DEV + local_index).astype(jnp.int32)


def draw_agglomerate(key, part):
    key_cuts = jax.random.fold_in(key, 21)
    key_names = jax.random.fold_in(key, 22)
    cuts = jax.random.permutation(key_cuts, NE - 1)[:NAGG - 1] + 1
    starts = jnp.zeros((NE,), jnp.int32).at[cuts].set(1)
    run_index = jnp.cumsum(starts).astype(jnp.int32)
    labels = jax.random.permutation(key_names, NAGG).astype(jnp.int32)
    return jnp.take(labels, run_index, axis=0).astype(jnp.int32)


def touch_ends(values, key, least, largest):
    place = [jax.random.randint(jax.random.fold_in(key, axis), (), 0, length) for axis, length in enumerate(values.shape)]
    longest = values.shape.index(max(values.shape))
    neighbour = place[:longest] + [(place[longest] + 1) % values.shape[longest]] + place[longest + 1:]
    return values.at[tuple(place)].set(least).at[tuple(neighbour)].set(largest)


def shard_levels(key, shape, shards, low, largest):
    factor_of = 1.0
    for axis_at, shards_of in shards:
        draws = jax.random.uniform(jax.random.fold_in(jax.random.fold_in(key, 6), axis_at), (shards_of,), jnp.float32, low / len(shards), largest / len(shards))
        factor_of = factor_of * jnp.repeat(jnp.exp(draws), shape[axis_at] // shards_of).reshape((-1,) + (1,) * (len(shape) - 1 - axis_at))
    return factor_of


def noise(stream_key, dims, width, reach, split=(), held_as=jnp.bfloat16):
    array = jax.random.normal(stream_key, dims, jnp.float32) * width
    if len(split) > 0:
        array = shard_levels(stream_key, dims, split, -0.22, 0.18) * array
    return jnp.clip(array, min=-reach, max=reach).astype(held_as)


def setup_inputs(seed: int = 0) -> dict:
    key_of = jax.random.split(jax.random.key(seed), 8)
    diagonal_block_list = noise(key_of[0], (NE, NB, NB), NB ** -0.5, 0.25, ((0, 8), (2, 4)))
    neighbour_block_list = noise(key_of[1], (NE, NBR, NB, NB), NB ** -0.5, 0.25, ((0, 8), (3, 4)))
    neighbours = draw_neighbours(jax.random.fold_in(key_of[7], 71), 0)
    damping = jnp.clip(jnp.exp(math.log(0.3) - 1.7917595 * jax.random.uniform(key_of[3], (NE, NB), jnp.float32) ** shard_levels(key_of[3], (NE, NB), ((0, 8), (1, 4)), -0.2, 0.2)), 0.05, 0.3)
    bases = noise(key_of[4], (NE, NB, NC), 0.2, 1.1953125, ((0, 8), (1, 4)))
    agglomerate = draw_agglomerate(jax.random.fold_in(key_of[7], 71), 0)
    group = touch_ends(jax.random.randint(key_of[6], (NAGG,), 0, NG), jax.random.fold_in(key_of[6], 1), 0, NG - 1).astype(jnp.int32)
    return dict(diagonal_block_list=diagonal_block_list, neighbour_block_list=neighbour_block_list, neighbours=neighbours, damping=damping, bases=bases, agglomerate=agglomerate, group=group)


def smooth_pass(source, diagonal_block_list, neighbour_block_list, neighbours, damping):
    def smooth_one(item):
        diag_part, nbr_part, neighbour_ids, own_rows, damp_rows = item
        nearby_elements = jnp.take(source, neighbour_ids, axis=0)
        total_result = jnp.dot(diag_part, own_rows, preferred_element_type=jnp.float32)
        total_result = total_result + jnp.einsum("kij,kjc->ic", nbr_part.astype(jnp.float32), nearby_elements.astype(jnp.float32))
        return (own_rows.astype(jnp.float32) - damp_rows[:, None] * total_result).astype(jnp.bfloat16)
    return lax.map(smooth_one, (diagonal_block_list, neighbour_block_list, neighbours, source, damping))


def reference(diagonal_block_list, neighbour_block_list, neighbours, damping, bases, agglomerate, group):
    present_value = bases
    for sweep_index in range(SWEEPS):
        present_value = smooth_pass(present_value, diagonal_block_list, neighbour_block_list, neighbours, damping)
    smoothed = present_value
    elem_group = jnp.take(group, agglomerate, axis=0)

    def couple_one(item):
        diag_part, nbr_part, neighbour_ids, own_rows, own_cluster, own_group = item
        left_diag = jnp.dot(own_rows.T, diag_part, preferred_element_type=jnp.float32).astype(jnp.bfloat16)
        left_nbr = jnp.einsum("ic,kis->kcs", own_rows.astype(jnp.float32), nbr_part.astype(jnp.float32)).astype(jnp.bfloat16)
        self_term = jnp.dot(left_diag, own_rows, preferred_element_type=jnp.float32)
        nearby_elements = jnp.take(smoothed, neighbour_ids, axis=0)
        nbr_terms = jnp.einsum("kcs,ksd->kcd", left_nbr.astype(jnp.float32), nearby_elements.astype(jnp.float32))
        same_cluster = (jnp.take(agglomerate, neighbour_ids, axis=0) == own_cluster).astype(jnp.float32)
        same_group = (jnp.take(elem_group, neighbour_ids, axis=0) == own_group).astype(jnp.float32)
        first_sum = self_term + jnp.sum(same_cluster[:, None, None] * nbr_terms, 0)
        second_level_sum = self_term + jnp.sum(same_group[:, None, None] * nbr_terms, 0)
        return first_sum, second_level_sum

    first_all, second_all = lax.map(couple_one, (diagonal_block_list, neighbour_block_list, neighbours, smoothed, agglomerate, elem_group))
    coarse = jax.ops.segment_sum(first_all, agglomerate, num_segments=NAGG)
    last_level = jax.ops.segment_sum(second_all, elem_group, num_segments=NG)
    return smoothed, coarse, last_level
```

```python
import functools

import jax
import jax.numpy as jnp
from jax import lax
from jax.experimental import pallas as pl
from jax.experimental.pallas import tpu as pltpu
from jax.sharding import PartitionSpec as P

SWEEPS = 2
NG = 8
VMEM = pl.BlockSpec(memory_space=pltpu.VMEM)
SMEM = pl.BlockSpec(memory_space=pltpu.SMEM)


def call(kernel, ins, outs, scratch, flops, *args):
    return pl.pallas_call(
        kernel,
        in_specs=ins,
        out_specs=[VMEM] * len(outs),
        out_shape=outs,
        scratch_shapes=scratch,
        compiler_params=pltpu.CompilerParams(vmem_limit_bytes=24 << 20),
        cost_estimate=pl.CostEstimate(flops=flops, bytes_accessed=4 << 20, transcendentals=0),
    )(*args)


def flip(x, axis, bit):
    size = lax.axis_size(axis)
    return lax.ppermute(x, axis, [(i, i ^ bit) for i in range(size) if i ^ bit < size])


def beside(x):
    size = lax.axis_size("elem")
    across = [(i, i + 1) for i in range(1, size - 1, 2)]
    return flip(x, "elem", 1), lax.ppermute(x, "elem", across + [(j, i) for i, j in across])


def scatter_sum(keep, send):
    bit = 1
    while True:
        total = keep + flip(send, "blk", bit)
        if total.shape[0] == 1:
            return total[0]
        keep, send = total[0::2], total[1::2].astype(jnp.bfloat16)
        bit *= 2


def gathered(x):
    parts = {0: x}
    bit = lax.axis_size("blk") // 2
    while bit:
        order = sorted(parts)
        other = flip(jnp.stack([parts[r] for r in order]), "blk", bit)
        for at, r in enumerate(order):
            parts[r + bit] = other[at]
        bit //= 2
    return jnp.stack([parts[r] for r in range(len(parts))])


def slot(pos_ref, element, count):
    position = pos_ref[0]
    offset = element - position * count
    even = position % 2 == 0
    below = jnp.where(even, 3 * count, 2 * count)
    above = jnp.where(even, 0, count)
    return offset + jnp.where(offset < 0, below, jnp.where(offset < count, 0, above))


def fill(slabs, own, pair, across):
    count = own.shape[0]
    slabs[0:count] = own[...]
    slabs[count : 2 * count] = pair[...]
    slabs[2 * count : 3 * count] = across[...]


def split_rows(pos_ref, value, part_ref, keep_ref, send_ref, at):
    chunks, rows = part_ref.shape[0], part_ref.shape[1]
    for j in range(chunks):
        part_ref[j] = value[j * rows : (j + 1) * rows]
    me = pos_ref[1]
    for r in range(chunks):
        chunk = part_ref[me ^ r]
        if r % 2 == 0:
            keep_ref[r // 2, at] = chunk
        else:
            send_ref[r // 2, at] = chunk.astype(send_ref.dtype)


def sweep_kernel(pos, nbrs, diag, blocks, own, pair, across, keep, send, slabs, part):
    count, faces = blocks.shape[0], blocks.shape[1]
    fill(slabs, own, pair, across)
    for i in range(count):
        left = [diag[i]] + [blocks[i, k] for k in range(faces)]
        right = [own[i]] + [slabs[slot(pos, nbrs[i, k], count)] for k in range(faces)]
        y = jnp.dot(
            jnp.concatenate(left, axis=1),
            jnp.concatenate(right, axis=0),
            preferred_element_type=jnp.float32,
        )
        split_rows(pos, y, part, keep, send, i)


def couple_kernel(
    pos, nbrs, agg, group, diag, blocks, every, pair, across, keep, send, slabs, part
):
    count, faces = blocks.shape[0], blocks.shape[1]
    width = pair.shape[2]
    fill(slabs, every.at[0], pair, across)
    first = pos[0] * count
    for i in range(count):
        rows = [every[pos[1] ^ j, i] for j in range(every.shape[0])]
        left = [diag[i]] + [blocks[i, k] for k in range(faces)]
        w = lax.dot_general(
            jnp.concatenate(rows, axis=0),
            jnp.concatenate(left, axis=1),
            (((0,), (0,)), ((), ())),
            preferred_element_type=jnp.float32,
        ).astype(jnp.bfloat16)
        own_agg = agg[first + i]
        own_group = group[own_agg]
        right = [jnp.concatenate([slabs[i], slabs[i]], axis=1)]
        for k in range(faces):
            near = nbrs[i, k]
            near_agg = agg[near]
            slab = slabs[slot(pos, near, count)]
            none = jnp.zeros_like(slab)
            right.append(
                jnp.concatenate(
                    [
                        jnp.where(near_agg == own_agg, slab, none),
                        jnp.where(group[near_agg] == own_group, slab, none),
                    ],
                    axis=1,
                )
            )
        t = jnp.dot(w, jnp.concatenate(right, axis=0), preferred_element_type=jnp.float32)
        split_rows(pos, t[:, :width], part, keep, send, i)
        split_rows(pos, t[:, width:], part, keep, send, count + i)


def pack_kernel(pos, agg, total, out, sums):
    count = total.shape[0] // 2
    owned = out.shape[1] - count
    sums[...] = jnp.zeros_like(sums)
    for i in range(count):
        at = agg[pos[0] * count + i]
        sums[at] = sums[at] + total[i]

    def one(dest, carry):
        for j in range(owned):
            out[dest, j] = sums[dest * owned + j].astype(out.dtype)
        out[dest, owned:] = total[count:].astype(out.dtype)
        return carry

    lax.fori_loop(0, out.shape[0], one, 0)


def finish_kernel(agg, group, parts, coarse, last, *, count):
    owned = coarse.shape[0]
    coarse[...] = jnp.zeros_like(coarse)
    last[...] = jnp.zeros_like(last)

    def one(source, carry):
        coarse[...] = coarse[...] + parts[source, :owned].astype(jnp.float32)
        for i in range(count):
            at = group[agg[source * count + i]]
            last[at] = last[at] + parts[source, owned + i].astype(jnp.float32)
        return carry

    lax.fori_loop(0, parts.shape[0], one, 0)


def body(diag, blocks, neighbours, damping, bases, agglomerate, group):
    count, rows, width = bases.shape
    faces = neighbours.shape[1]
    ways = lax.axis_size("blk")
    size = lax.axis_size("elem")
    pos = jnp.stack([lax.axis_index("elem"), lax.axis_index("blk")]).astype(jnp.int32)
    f32, bf16 = jnp.float32, jnp.bfloat16
    slabs = pltpu.VMEM((3 * count, rows, width), bf16)
    shape = jax.ShapeDtypeStruct
    flops = 2 * count * (faces + 1) * ways * rows * rows * width

    x = bases
    pair, across = beside(x)
    for _ in range(SWEEPS):
        keep, send = call(
            sweep_kernel,
            [SMEM, SMEM] + [VMEM] * 5,
            [
                shape((ways // 2, count, rows, width), f32),
                shape((ways // 2, count, rows, width), bf16),
            ],
            [slabs, pltpu.VMEM((ways, rows, width), f32)],
            flops,
            *(pos, neighbours, diag, blocks, x, pair, across),
        )
        total = scatter_sum(keep, send)
        x = (x.astype(f32) - damping[:, :, None] * total).astype(bf16)
        pair, across = beside(x)

    every = gathered(x)
    part = width // ways
    keep, send = call(
        couple_kernel,
        [SMEM] * 4 + [VMEM] * 5,
        [
            shape((ways // 2, 2 * count, part, width), f32),
            shape((ways // 2, 2 * count, part, width), bf16),
        ],
        [slabs, pltpu.VMEM((ways, part, width), f32)],
        flops,
        *(pos, neighbours, agglomerate, group, diag, blocks, every, pair, across),
    )
    total = scatter_sum(keep, send)

    owned = group.shape[0] // size
    (parts,) = call(
        pack_kernel,
        [SMEM, SMEM, VMEM],
        [shape((size, owned + count, part, width), bf16)],
        [pltpu.VMEM((group.shape[0], part, width), f32)],
        1 << 20,
        *(pos, agglomerate, total),
    )
    parts = lax.all_to_all(parts, "elem", 0, 0, tiled=True)
    coarse, last = call(
        functools.partial(finish_kernel, count=count),
        [SMEM, SMEM, VMEM],
        [shape((owned, part, width), f32), shape((NG, part, width), f32)],
        [],
        1 << 20,
        *(agglomerate, group, parts),
    )
    return x, coarse, last


def solution(mesh):
    return jax.shard_map(
        body,
        mesh=mesh,
        in_specs=(
            P("elem", None, "blk"),
            P("elem", None, None, "blk"),
            P("elem", None),
            P("elem", "blk"),
            P("elem", "blk", None),
            P(),
            P(),
        ),
        out_specs=(P("elem", "blk", None), P("elem", "blk", None), P(None, "blk", None)),
        check_vma=False,
    )
```

```python
import functools

import jax
import jax.numpy as jnp
from jax import lax
from jax.experimental import pallas as pl
from jax.experimental.pallas import tpu as pltpu
from jax.sharding import PartitionSpec as P


SWEEPS = 2
NG = 8
VMEM = pl.BlockSpec(memory_space=pltpu.VMEM)
SMEM = pl.BlockSpec(memory_space=pltpu.SMEM)
ANY = pl.BlockSpec(memory_space=pl.ANY)
DIRECT = 3


def call(kernel, ins, outs, scratch, flops, *args):
    return pl.pallas_call(
        kernel,
        in_specs=ins,
        out_specs=[VMEM] * len(outs),
        out_shape=outs,
        scratch_shapes=scratch,
        compiler_params=pltpu.CompilerParams(vmem_limit_bytes=24 << 20),
        cost_estimate=pl.CostEstimate(flops=flops, bytes_accessed=4 << 20, transcendentals=0),
    )(*args)


def flip(x, axis, bit):
    size = lax.axis_size(axis)
    return lax.ppermute(x, axis, [(i, i ^ bit) for i in range(size) if i ^ bit < size])


def beside(x):
    size = lax.axis_size("elem")
    ring = [(i, (i + 1) % size) for i in range(size)]
    before = lax.ppermute(x, "elem", ring)
    after = lax.ppermute(x, "elem", [(j, i) for i, j in ring])
    return before, after


def scatter_sum(keep, send):
    bit = 1
    while True:
        total = keep + flip(send, "blk", bit)
        if total.shape[0] == 1:
            return total[0]
        keep, send = total[0::2], total[1::2].astype(jnp.bfloat16)
        bit *= 2


def gathered(x):
    parts = {0: x}
    bit = lax.axis_size("blk") // 2
    while bit:
        order = sorted(parts)
        other = flip(jnp.stack([parts[r] for r in order]), "blk", bit)
        for at, r in enumerate(order):
            parts[r + bit] = other[at]
        bit //= 2
    return jnp.stack([parts[r] for r in range(len(parts))])


def slot(pos_ref, element, count):
    return element - (pos_ref[0] - 1) * count


def fill(slabs, own, before, after):
    count = own.shape[0]
    slabs[0:count] = before[...]
    slabs[count : 2 * count] = own[...]
    slabs[2 * count : 3 * count] = after[...]


def split_rows(pos_ref, value, part_ref, keep_ref, send_ref, at):
    chunks, rows = part_ref.shape[0], part_ref.shape[1]
    for j in range(chunks):
        part_ref[j] = value[j * rows : (j + 1) * rows]
    me = pos_ref[1]
    for r in range(chunks):
        chunk = part_ref[me ^ r]
        if r % 2 == 0:
            keep_ref[r // 2, at] = chunk
        else:
            send_ref[r // 2, at] = chunk.astype(send_ref.dtype)


def stage_kernel(diag, blocks, diag_out, blocks_out, sems):
    count = diag.shape[0]
    copies = []
    for i in range(count):
        copies.append(pltpu.make_async_copy(diag.at[i], diag_out.at[i], sems.at[2 * i]))
        copies.append(pltpu.make_async_copy(blocks.at[i], blocks_out.at[i], sems.at[2 * i + 1]))
    for copy in copies:
        copy.start()
    for copy in copies:
        copy.wait()


def sweep_kernel(pos, nbrs, diag, blocks, own, before, after, keep, send, slabs, part):
    count, faces = blocks.shape[0], blocks.shape[1]
    fill(slabs, own, before, after)
    for i in range(count):
        left = [diag[i]] + [blocks[i, k] for k in range(faces)]
        right = [own[i]] + [slabs[slot(pos, nbrs[i, k], count)] for k in range(faces)]
        y = jnp.dot(
            jnp.concatenate(left, axis=1),
            jnp.concatenate(right, axis=0),
            preferred_element_type=jnp.float32,
        )
        split_rows(pos, y, part, keep, send, i)


def left_kernel(pos, diag, blocks, every, w):
    count, faces = blocks.shape[0], blocks.shape[1]
    for i in range(count):
        rows = [every[pos[1] ^ j, i] for j in range(every.shape[0])]
        left = [diag[i]] + [blocks[i, k] for k in range(faces)]
        w[i] = lax.dot_general(
            jnp.concatenate(rows, axis=0),
            jnp.concatenate(left, axis=1),
            (((0,), (0,)), ((), ())),
            preferred_element_type=jnp.float32,
        ).astype(w.dtype)


def couple_kernel(pos, nbrs, agg, group, w, own, before, after, keep, send, slabs, part):
    count, width = own.shape[0], own.shape[2]
    faces = w.shape[2] // own.shape[1] - 1
    fill(slabs, own, before, after)
    first = pos[0] * count
    for i in range(count):
        own_agg = agg[first + i]
        own_group = group[own_agg]
        right = [jnp.concatenate([own[i], own[i]], axis=1)]
        for k in range(faces):
            near = nbrs[i, k]
            near_agg = agg[near]
            slab = slabs[slot(pos, near, count)]
            none = jnp.zeros_like(slab)
            right.append(
                jnp.concatenate(
                    [
                        jnp.where(near_agg == own_agg, slab, none),
                        jnp.where(group[near_agg] == own_group, slab, none),
                    ],
                    axis=1,
                )
            )
        t = jnp.dot(w[i], jnp.concatenate(right, axis=0), preferred_element_type=jnp.float32)
        split_rows(pos, t[:, :width], part, keep, send, i)
        split_rows(pos, t[:, width:], part, keep, send, count + i)


def merge_kernel(pos, agg, group, *refs):
    raws, (coarse, last, send) = refs[:-3], refs[-3:]
    count = raws[0].shape[0] // 2
    owned, groups = coarse.shape[0], last.shape[0]
    mine = [0.0] * owned
    theirs = [0.0] * owned
    level = [0.0] * groups
    for k, raw in enumerate(raws):
        source = (pos[0] ^ (2 * k)) * count
        for i in range(count):
            at = agg[source + i]
            value = raw[i].astype(jnp.float32)
            for j in range(owned):
                mine[j] += jnp.where(at == pos[0] * owned + j, value, 0.0)
                theirs[j] += jnp.where(at == (pos[0] ^ 1) * owned + j, value, 0.0)
            value = raw[count + i].astype(jnp.float32)
            for g in range(groups):
                level[g] += jnp.where(group[at] == g, value, 0.0)
    for j in range(owned):
        coarse[j] = mine[j]
        send[j] = theirs[j].astype(send.dtype)
    for g in range(groups):
        last[g] = level[g]
        send[owned + g] = level[g].astype(send.dtype)


def pack_kernel(pos, agg, total, out, sums):
    count = total.shape[0] // 2
    owned = out.shape[1] - count
    sums[...] = jnp.zeros_like(sums)
    for i in range(count):
        at = agg[pos[0] * count + i]
        sums[at] = sums[at] + total[i]

    def one(dest, carry):
        for j in range(owned):
            out[dest, j] = sums[dest * owned + j].astype(out.dtype)
        out[dest, owned:] = total[count:].astype(out.dtype)
        return carry

    lax.fori_loop(0, out.shape[0], one, 0)


def finish_kernel(agg, group, parts, coarse, last, *, count):
    owned = coarse.shape[0]
    coarse[...] = jnp.zeros_like(coarse)
    last[...] = jnp.zeros_like(last)

    def one(source, carry):
        coarse[...] = coarse[...] + parts[source, :owned].astype(jnp.float32)
        for i in range(count):
            at = group[agg[source * count + i]]
            last[at] = last[at] + parts[source, owned + i].astype(jnp.float32)
        return carry

    lax.fori_loop(0, parts.shape[0], one, 0)


def direct_tail(pos, agglomerate, group, total):
    size = lax.axis_size("elem")
    owned = group.shape[0] // size
    _, part, width = total.shape
    shape = jax.ShapeDtypeStruct
    raw = total.astype(jnp.bfloat16)
    raws = [raw]
    for k in range(2, size, 2):
        raws.append(flip(raw, "elem", k))
    coarse, last, send = call(
        merge_kernel,
        [SMEM] * 3 + [VMEM] * len(raws),
        [
            shape((owned, part, width), jnp.float32),
            shape((NG, part, width), jnp.float32),
            shape((owned + NG, part, width), jnp.bfloat16),
        ],
        [],
        1 << 20,
        *(pos, agglomerate, group, *raws),
    )
    received = flip(send, "elem", 1)
    return coarse + received[:owned], last + received[owned:]


def routed_tail(pos, agglomerate, group, total):
    size = lax.axis_size("elem")
    owned = group.shape[0] // size
    count, part, width = total.shape[0] // 2, total.shape[1], total.shape[2]
    shape = jax.ShapeDtypeStruct
    (parts,) = call(
        pack_kernel,
        [SMEM, SMEM, VMEM],
        [shape((size, owned + count, part, width), jnp.bfloat16)],
        [pltpu.VMEM((group.shape[0], part, width), jnp.float32)],
        1 << 20,
        *(pos, agglomerate, total),
    )
    parts = lax.all_to_all(parts, "elem", 0, 0, tiled=True)
    return call(
        functools.partial(finish_kernel, count=count),
        [SMEM, SMEM, VMEM],
        [shape((owned, part, width), jnp.float32), shape((NG, part, width), jnp.float32)],
        [],
        1 << 20,
        *(agglomerate, group, parts),
    )


def steps(diag, blocks, neighbours, damping, bases, agglomerate, group):
    count, rows, width = bases.shape
    faces = neighbours.shape[1]
    ways = lax.axis_size("blk")
    size = lax.axis_size("elem")
    pos = jnp.stack([lax.axis_index("elem"), lax.axis_index("blk")]).astype(jnp.int32)
    f32, bf16 = jnp.float32, jnp.bfloat16
    slabs = pltpu.VMEM((3 * count, rows, width), bf16)
    shape = jax.ShapeDtypeStruct
    flops = 2 * count * (faces + 1) * ways * rows * rows * width

    x = bases
    before, after = beside(x)
    diag, blocks = call(
        stage_kernel,
        [ANY, ANY],
        [shape(diag.shape, bf16), shape(blocks.shape, bf16)],
        [pltpu.SemaphoreType.DMA((2 * count,))],
        flops,
        *(diag, blocks),
    )
    for sweep in range(SWEEPS):
        keep, send = call(
            sweep_kernel,
            [SMEM, SMEM] + [VMEM] * 5,
            [
                shape((ways // 2, count, rows, width), f32),
                shape((ways // 2, count, rows, width), bf16),
            ],
            [slabs, pltpu.VMEM((ways, rows, width), f32)],
            flops,
            *(pos, neighbours, diag, blocks, x, before, after),
        )
        total = scatter_sum(keep, send)
        x = (x.astype(f32) - damping[:, :, None] * total).astype(bf16)
        if sweep + 1 < SWEEPS:
            before, after = beside(x)

    every = gathered(x)
    before, after = beside(x)
    (w,) = call(
        left_kernel,
        [SMEM] + [VMEM] * 3,
        [shape((count, width, (faces + 1) * rows), bf16)],
        [],
        flops,
        *(pos, diag, blocks, every),
    )
    part = width // ways
    keep, send = call(
        couple_kernel,
        [SMEM] * 4 + [VMEM] * 4,
        [
            shape((ways // 2, 2 * count, part, width), f32),
            shape((ways // 2, 2 * count, part, width), bf16),
        ],
        [slabs, pltpu.VMEM((ways, part, width), f32)],
        flops,
        *(pos, neighbours, agglomerate, group, w, x, before, after),
    )
    total = scatter_sum(keep, send)
    tail = direct_tail if size % 2 == 0 and size // 2 - 1 <= DIRECT else routed_tail
    coarse, last = tail(pos, agglomerate, group, total)
    return x, coarse, last


def solution(mesh):
    return jax.shard_map(
        steps,
        mesh=mesh,
        in_specs=(
            P("elem", None, "blk"),
            P("elem", None, None, "blk"),
            P("elem", None),
            P("elem", "blk"),
            P("elem", "blk", None),
            P(),
            P(),
        ),
        out_specs=(P("elem", "blk", None), P("elem", "blk", None), P(None, "blk", None)),
        check_vma=False,
    )
```

```python
import functools

import jax
import jax.numpy as jnp
from jax import lax
from jax.experimental import pallas as pl
from jax.experimental.pallas import tpu as pltpu
from jax.sharding import PartitionSpec as P


SWEEPS = 2
NG = 8
VMEM = pl.BlockSpec(memory_space=pltpu.VMEM)
SMEM = pl.BlockSpec(memory_space=pltpu.SMEM)
ANY = pl.BlockSpec(memory_space=pl.ANY)
DIRECT = 3


def call(kernel, ins, outs, scratch, flops, *args, place=VMEM):
    return pl.pallas_call(
        kernel,
        in_specs=ins,
        out_specs=[place] * len(outs),
        out_shape=outs,
        scratch_shapes=scratch,
        compiler_params=pltpu.CompilerParams(vmem_limit_bytes=24 << 20),
        cost_estimate=pl.CostEstimate(flops=flops, bytes_accessed=4 << 20, transcendentals=0),
    )(*args)


def flip(x, axis, bit):
    size = lax.axis_size(axis)
    return lax.ppermute(x, axis, [(i, i ^ bit) for i in range(size) if i ^ bit < size])


def whole_pairs(target):
    size, ways = lax.axis_size("elem"), lax.axis_size("blk")
    pairs = []
    for p in range(size):
        for b in range(ways):
            q, c = target(p, b)
            inside = 0 <= q < size
            pairs.append((p * ways + b, q * ways + c if inside else p * ways + (b ^ 1)))
    return pairs


def beside(x):
    axes = ("elem", "blk")
    one = lax.ppermute(x, axes, whole_pairs(lambda p, b: (p ^ 1, b)))
    two = lax.ppermute(x, axes, whole_pairs(lambda p, b: (p - 1 + 2 * (p % 2), b)))
    return one, two


def swapped():
    return 1 - lax.axis_index("elem") % 2


def halved(keep, send):
    bit = 1
    while True:
        other = flip(send, "blk", bit)
        total = keep + other
        if total.shape[0] == 2:
            return total
        keep, send = total[0::2], total[1::2].astype(jnp.bfloat16)
        bit *= 2


def gathered(x, opposite):
    bit = lax.axis_size("blk") // 2
    parts = {0: x, bit: opposite}
    bit //= 2
    while bit:
        order = sorted(parts)
        other = flip(jnp.stack([parts[r] for r in order]), "blk", bit)
        for at, r in enumerate(order):
            parts[r + bit] = other[at]
        bit //= 2
    return jnp.stack([parts[r] for r in range(len(parts))])


def slot(pos_ref, element, count):
    offset = element - pos_ref[0] * count
    turn = jnp.where(offset < 0, 2 * count, jnp.where(offset < count, 0, -2 * count))
    return offset + count + pos_ref[2] * turn


def fill(slabs, pieces):
    at = 0
    for piece in pieces:
        slabs[at : at + piece.shape[0]] = piece[...]
        at += piece.shape[0]


def split_rows(pos_ref, value, part_ref, keep_ref, send_ref, at):
    chunks, rows = part_ref.shape[0], part_ref.shape[1]
    for j in range(chunks):
        part_ref[j] = value[j * rows : (j + 1) * rows]
    me = pos_ref[1]
    for r in range(chunks):
        chunk = part_ref[me ^ r]
        if r % 2 == 0:
            keep_ref[r // 2, at] = chunk
        else:
            send_ref[r // 2, at] = chunk.astype(send_ref.dtype)


def stage_kernel(_, diag, blocks, bases, diag_out, blocks_out, bases_out, sems):
    count = diag.shape[0]
    copies = [pltpu.make_async_copy(bases, bases_out, sems.at[2 * count])]
    for i in range(count):
        copies.append(pltpu.make_async_copy(diag.at[i], diag_out.at[i], sems.at[2 * i]))
        copies.append(pltpu.make_async_copy(blocks.at[i], blocks_out.at[i], sems.at[2 * i + 1]))
    for copy in copies:
        copy.start()
    for copy in copies:
        copy.wait()


def product(pos, nbrs, diag, blocks, slabs, out, parity):
    count, faces = blocks.shape[0], blocks.shape[1]
    rows = slabs.shape[1]
    for i in range(count):
        left = []
        for r in range(parity, 2 * out.shape[0], 2):
            cut = pl.ds(pl.multiple_of((pos[1] ^ r) * rows, rows), rows)
            line = [diag[i, cut, :]] + [blocks[i, k, cut, :] for k in range(faces)]
            left.append(jnp.concatenate(line, axis=1))
        right = [slabs[count + i]] + [slabs[slot(pos, nbrs[i, k], count)] for k in range(faces)]
        y = jnp.dot(
            jnp.concatenate(left, axis=0),
            jnp.concatenate(right, axis=0),
            preferred_element_type=jnp.float32,
        )
        for r in range(out.shape[0]):
            out[r, i] = y[r * rows : (r + 1) * rows].astype(out.dtype)


def send_kernel(pos, nbrs, diag, blocks, *refs):
    pieces, (send, slabs) = refs[:-2], refs[-2:]
    fill(slabs, pieces)
    product(pos, nbrs, diag, blocks, slabs, send, 1)


def keep_kernel(pos, nbrs, diag, blocks, slabs, keep):
    product(pos, nbrs, diag, blocks, slabs, keep, 0)


def left_kernel(pos, diag, blocks, every, w):
    count, faces = blocks.shape[0], blocks.shape[1]
    for i in range(count):
        rows = [every[pos[1] ^ j, i] for j in range(every.shape[0])]
        left = [diag[i]] + [blocks[i, k] for k in range(faces)]
        w[i] = lax.dot_general(
            jnp.concatenate(rows, axis=0),
            jnp.concatenate(left, axis=1),
            (((0,), (0,)), ((), ())),
            preferred_element_type=jnp.float32,
        ).astype(w.dtype)


def couple_kernel(pos, nbrs, agg, group, w, *refs):
    pieces, (keep, send, slabs, part) = refs[:-4], refs[-4:]
    count, width = w.shape[0], w.shape[1]
    faces = w.shape[2] // slabs.shape[1] - 1
    fill(slabs, pieces)
    first = pos[0] * count
    for i in range(count):
        own_agg = agg[first + i]
        own_group = group[own_agg]
        right = [jnp.concatenate([slabs[count + i]] * 2, axis=1)]
        for k in range(faces):
            near = nbrs[i, k]
            near_agg = agg[near]
            slab = slabs[slot(pos, near, count)]
            none = jnp.zeros_like(slab)
            right.append(
                jnp.concatenate(
                    [
                        jnp.where(near_agg == own_agg, slab, none),
                        jnp.where(group[near_agg] == own_group, slab, none),
                    ],
                    axis=1,
                )
            )
        t = jnp.dot(w[i], jnp.concatenate(right, axis=0), preferred_element_type=jnp.float32)
        split_rows(pos, t[:, :width], part, keep, send, i)
        split_rows(pos, t[:, width:], part, keep, send, count + i)


def merge_kernel(pos, agg, group, kept, opposite, pair, across, coarse, last, *sends):
    count = kept.shape[0] // 2
    owned, groups = coarse.shape[0], last.shape[0]
    sums = [[0.0] * owned for _ in range(len(sends) + 1)]
    level = [0.0] * groups
    for flipped in range(2):
        for i in range(2 * count):
            if flipped:
                value = pair[i].astype(jnp.float32) + across[i].astype(jnp.float32)
            else:
                value = kept[i] + opposite[i].astype(jnp.float32)
            at = agg[(pos[0] ^ flipped) * count + i % count]
            if i < count:
                for k in range(len(sums)):
                    for j in range(owned):
                        here = at == (pos[0] ^ (2 * k)) * owned + j
                        sums[k][j] += jnp.where(here, value, 0.0)
            else:
                for g in range(groups):
                    level[g] += jnp.where(group[at] == g, value, 0.0)
    for j in range(owned):
        coarse[j] = sums[0][j]
        for k, send in enumerate(sends):
            send[j] = sums[k + 1][j].astype(send.dtype)
    for g in range(groups):
        last[g] = level[g]
        for send in sends:
            send[owned + g] = level[g].astype(send.dtype)


def close_kernel(coarse, last, *refs):
    received, (coarse_hbm, last_hbm, coarse_sum, last_sum, sems) = refs[:-5], refs[-5:]
    owned = coarse.shape[0]
    total = coarse[...]
    for part in received:
        total += part[:owned].astype(jnp.float32)
    coarse_sum[...] = total
    total = last[...]
    for part in received:
        total += part[owned:].astype(jnp.float32)
    last_sum[...] = total
    first = pltpu.make_async_copy(coarse_sum, coarse_hbm, sems.at[0])
    second = pltpu.make_async_copy(last_sum, last_hbm, sems.at[1])
    first.start()
    second.start()
    first.wait()
    second.wait()


def pack_kernel(pos, agg, total, out, sums):
    count = total.shape[0] // 2
    owned = out.shape[1] - count
    sums[...] = jnp.zeros_like(sums)
    for i in range(count):
        at = agg[pos[0] * count + i]
        sums[at] = sums[at] + total[i]

    def one(dest, carry):
        for j in range(owned):
            out[dest, j] = sums[dest * owned + j].astype(out.dtype)
        out[dest, owned:] = total[count:].astype(out.dtype)
        return carry

    lax.fori_loop(0, out.shape[0], one, 0)


def finish_kernel(agg, group, parts, coarse, last, *, count):
    owned = coarse.shape[0]
    coarse[...] = jnp.zeros_like(coarse)
    last[...] = jnp.zeros_like(last)

    def one(source, carry):
        coarse[...] = coarse[...] + parts[source, :owned].astype(jnp.float32)
        for i in range(count):
            at = group[agg[source * count + i]]
            last[at] = last[at] + parts[source, owned + i].astype(jnp.float32)
        return carry

    lax.fori_loop(0, parts.shape[0], one, 0)


def direct_tail(pos, agglomerate, group, total):
    size, ways = lax.axis_size("elem"), lax.axis_size("blk")
    owned = group.shape[0] // size
    _, _, part, width = total.shape
    shape = jax.ShapeDtypeStruct
    bf16, f32 = jnp.bfloat16, jnp.float32
    half = ways // 2
    own, other = total[0].astype(bf16), total[1].astype(bf16)
    cross = [
        (p * ways + b, (p ^ 1) * ways + (b ^ half)) for p in range(size) for b in range(ways)
    ]
    opposite = flip(other, "blk", half)
    pair = flip(own, "elem", 1)
    across = lax.ppermute(other, ("elem", "blk"), cross)
    line = range(2, size, 2)
    packed = shape((owned + NG, part, width), bf16)
    coarse, last, *sends = call(
        merge_kernel,
        [SMEM] * 3 + [VMEM] * 4,
        [shape((owned, part, width), f32), shape((NG, part, width), f32)] + [packed] * len(line),
        [],
        1 << 20,
        *(pos, agglomerate, group, total[0], opposite, pair, across),
    )
    received = [flip(send, "elem", k) for k, send in zip(line, sends)]
    return call(
        close_kernel,
        [VMEM] * (2 + len(received)),
        [shape(coarse.shape, f32), shape(last.shape, f32)],
        [
            pltpu.VMEM(coarse.shape, f32),
            pltpu.VMEM(last.shape, f32),
            pltpu.SemaphoreType.DMA((2,)),
        ],
        1 << 20,
        *(coarse, last, *received),
        place=ANY,
    )


def routed_tail(pos, agglomerate, group, total):
    size = lax.axis_size("elem")
    owned = group.shape[0] // size
    total = total[0] + flip(total[1].astype(jnp.bfloat16), "blk", lax.axis_size("blk") // 2)
    count, part, width = total.shape[0] // 2, total.shape[1], total.shape[2]
    shape = jax.ShapeDtypeStruct
    (parts,) = call(
        pack_kernel,
        [SMEM, SMEM, VMEM],
        [shape((size, owned + count, part, width), jnp.bfloat16)],
        [pltpu.VMEM((group.shape[0], part, width), jnp.float32)],
        1 << 20,
        *(pos, agglomerate, total),
    )
    parts = lax.all_to_all(parts, "elem", 0, 0, tiled=True)
    return call(
        functools.partial(finish_kernel, count=count),
        [SMEM, SMEM, VMEM],
        [shape((owned, part, width), jnp.float32), shape((NG, part, width), jnp.float32)],
        [],
        1 << 20,
        *(agglomerate, group, parts),
    )


def steps(diag, blocks, neighbours, damping, bases, agglomerate, group):
    count, rows, width = bases.shape
    faces = neighbours.shape[1]
    ways = lax.axis_size("blk")
    size = lax.axis_size("elem")
    pos = jnp.stack([lax.axis_index("elem"), lax.axis_index("blk"), swapped()]).astype(jnp.int32)
    f32, bf16 = jnp.float32, jnp.bfloat16
    shape = jax.ShapeDtypeStruct
    flops = 2 * count * (faces + 1) * ways * rows * rows * width

    first, second = beside(bases)
    diag, blocks, x = call(
        stage_kernel,
        [SMEM] + [ANY] * 3,
        [shape(diag.shape, bf16), shape(blocks.shape, bf16), shape(bases.shape, bf16)],
        [pltpu.SemaphoreType.DMA((2 * count + 1,))],
        flops,
        *(pos, diag, blocks, bases),
    )
    half = ways // 2
    for sweep in range(SWEEPS):
        send, slabs = call(
            send_kernel,
            [SMEM, SMEM] + [VMEM] * 5,
            [
                shape((half, count, rows, width), bf16),
                shape((3 * count, rows, width), bf16),
            ],
            [],
            flops // 2,
            *(pos, neighbours, diag, blocks, first, x, second),
        )
        (keep,) = call(
            keep_kernel,
            [SMEM, SMEM] + [VMEM] * 3,
            [shape((half, count, rows, width), f32)],
            [],
            flops // 2,
            *(pos, neighbours, diag, blocks, slabs),
        )
        total = halved(keep, send)
        y = total[0] + flip(total[1].astype(bf16), "blk", half)
        x = (x.astype(f32) - damping[:, :, None] * y).astype(bf16)
        if sweep + 1 == SWEEPS:
            opposite = flip(x, "blk", half)
        first, second = beside(x)

    every = gathered(x, opposite)
    (w,) = call(
        left_kernel,
        [SMEM] + [VMEM] * 3,
        [shape((count, width, (faces + 1) * rows), bf16)],
        [],
        flops,
        *(pos, diag, blocks, every),
    )
    part = width // ways
    keep, send = call(
        couple_kernel,
        [SMEM] * 4 + [VMEM] * 4,
        [
            shape((ways // 2, 2 * count, part, width), f32),
            shape((ways // 2, 2 * count, part, width), bf16),
        ],
        [pltpu.VMEM((3 * count, rows, width), bf16), pltpu.VMEM((ways, part, width), f32)],
        flops,
        *(pos, neighbours, agglomerate, group, w, first, x, second),
    )
    total = halved(keep, send)
    tail = direct_tail if size % 2 == 0 and size // 2 - 1 <= DIRECT else routed_tail
    coarse, last = tail(pos, agglomerate, group, total)
    return x, coarse, last


def solution(mesh):
    return jax.shard_map(
        steps,
        mesh=mesh,
        in_specs=(
            P("elem", None, "blk"),
            P("elem", None, None, "blk"),
            P("elem", None),
            P("elem", "blk"),
            P("elem", "blk", None),
            P(),
            P(),
        ),
        out_specs=(P("elem", "blk", None), P("elem", "blk", None), P(None, "blk", None)),
        check_vma=False,
    )
```
